32 devices in a mesh: section: 4 (over y, x), expert: 8 (over z, core).
Axes of the slice: x: 2, y: 2, z: 4, core: 2. Of those that a mesh axis runs over, the one named last changes fastest.
Arguments:
- section_inputs: float32 [4, 1024, 2048], P('section', 'expert'), may hold values from -6 to 6
- stored_inputs: float32 [4, 1024, 2048], P('section', 'expert'), may hold values from -6 to 6
- out_grads: bfloat16 [4, 1024, 2048], P('section', 'expert'), may hold values from -6 to 6
- fwd_routes: int32 [4, 1024, 2], P('section', 'expert'), may hold values from 0 to 3, all different within a row; in each aligned block of 128 rows (0 to 127, 128 to 255, ..., all dimensions but the last counted through in order) at most 80 rows name the same one
- fwd_gates: float32 [4, 1024, 2], P('section', 'expert'), may hold values from 0.2 to 1
- fwd_modulation: float32 [4, 3, 2048], P('section'), may hold values from -3 to 3
- bwd_routes: int32 [4, 1024, 2], P('section', 'expert'), may hold values from 0 to 3, all different within a row; in each aligned block of 128 rows (0 to 127, 128 to 255, ..., all dimensions but the last counted through in order) at most 80 rows name the same one
- bwd_gates: float32 [4, 1024, 2], P('section', 'expert'), may hold values from 0.2 to 1
- bwd_modulation: float32 [4, 3, 2048], P('section'), may hold values from -3 to 3
- up_weight: bfloat16 [4, 8, 2048, 1024], P('section', 'expert'), may hold values from -0.125 to 0.125
- down_weight: bfloat16 [4, 8, 1024, 2048], P('section', 'expert'), may hold values from -0.125 to 0.125
Outputs:
- next_inputs: float32 [4, 1024, 2048], P('section', 'expert')
- input_grads: bfloat16 [4, 1024, 2048], P('section', 'expert')
The draws below stay inside these ranges and needn't reach their ends.
Inputs may be any that keep to these rules, and one draw needn't show every extreme that they name: `fwd_routes`: A token names two different experts. In the rows of one index of expert (aligned blocks of 128 rows of a section) no expert is named more than 80 times, a bound that some block reaches. `bwd_routes`: A token names two different experts. In the rows of one index of expert (aligned blocks of 128 rows of a section) no expert is named more than 80 times, a bound that some block reaches.
All inputs are finite; a program needn't handle non-finite values.
Results may differ from the reference program's by a relative error of at most 0.0042.
Values may be sent and summed in bfloat16 or wider, within the bound.
A program may use at most 128 MiB of HBM per device.

```python
import math
import jax
import jax.numpy as jnp
import numpy as np
from jax import lax

D = 2048
FF = 2048
FF_DEV = 1024
TOK_DEV = 128
TOKENS = 1024
EXPERTS = 4
CAP = 80
N_SECTION = 4
N_EXPERT = 8


def levels(rng, dims, split, smallest, top_value):
    def one(position, shards_of):
        draws = jax.random.uniform(jax.random.fold_in(jax.random.fold_in(rng, 6), position), (shards_of,), jnp.float32, smallest / len(split), top_value / len(split))
        return jnp.repeat(jnp.exp(draws), dims[position] // shards_of).reshape((-1,) + (1,) * (len(dims) - position - 1))

    gain = one(*split[0])
    for cut in split[1:]:
        gain = gain * one(*cut)
    return gain


def routed_block(key, own, number, rows, number_of, top, limit, lean):
    ranking = jax.random.permutation(key, number_of)
    crowded, ordinary = load_shares(number_of, rows * top, limit, lean, True), load_shares(number_of, rows * top, limit, lean, False)
    places = jnp.arange(number_of)

    def named(tallies, turn):
        used = int((tallies > 0).sum())
        fixed = max(1, used // 4)
        passed = fixed + (places - fixed + turn * (used - fixed)) % max(1, number_of - fixed)
        return jnp.zeros((number_of,), jnp.int32).at[ranking[jnp.where(places < fixed, places, passed)]].set(jnp.asarray(tallies, jnp.int32))

    tallies = jnp.where(number % 4 == 0, named(crowded, number // 4), named(ordinary, number - number // 4 - 1))
    mixed = jax.random.permutation(jax.random.fold_in(own, 3), number_of)
    giver, receiver = mixed[0:number_of // 2 * 2:2], mixed[1:number_of // 2 * 2:2]
    slack = jnp.minimum(tallies[giver] - 1, limit - tallies[receiver]) // 2
    slack = jnp.where((giver == ranking[0]) | (receiver == ranking[0]) | (tallies[receiver] == 0), 0, jnp.maximum(slack, 0))
    passed = jax.random.randint(jax.random.fold_in(own, 4), (number_of // 2,), 0, 1 << 20) % (slack + 1)
    tallies = tallies.at[giver].add(-passed).at[receiver].add(passed)
    items = jnp.searchsorted(jnp.cumsum(tallies), jnp.arange(rows * top), side="right").astype(jnp.int32)
    table = items.reshape(top, rows).T
    table = table[jax.random.permutation(jax.random.fold_in(own, 1), rows)]
    turn = jax.random.randint(jax.random.fold_in(own, 2), (rows, 1), 0, top)
    return jnp.take_along_axis(table, (jnp.arange(top)[None, :] + turn) % top, axis=1)


def load_shares(count, total, most, slope, full):
    weights = [(1 << 20) // math.isqrt(standing ** slope) + 1 for standing in range(1, count + 1)]
    largest = most if full else min(most, max(-(-total // count), total * weights[0] // sum(weights)))
    least = 1 if total - largest >= count - 1 else 0
    counts, rest = [largest] + [least] * (count - 1), total - largest - least * (count - 1)
    while rest > 0:
        movable = [i for i in range(1, count) if counts[i] < largest] or [i for i in range(1, count) if counts[i] < most]
        whole, remaining = sum([weights[i] for i in movable]), rest
        for i in movable:
            more = min(most - counts[i], max(1, remaining * weights[i] // whole), rest)
            counts[i] = counts[i] + more
            rest = rest - more
    return np.array(counts)


def normal_values(stream_key, dims, width, most, split=(), held_as=jnp.bfloat16):
    drawn = width * jax.random.normal(stream_key, dims, jnp.float32)
    if split:
        drawn = drawn * levels(stream_key, dims, split, -0.22, 0.18)
    return jnp.clip(drawn, -most, most).astype(held_as)


def setup_inputs(seed: int = 0) -> dict:
    keys = jax.random.split(jax.random.key(seed), 12)
    section_inputs = normal_values(keys[0], (N_SECTION, TOKENS, D), 1.0, 6.0, ((0, 4), (1, 8)), jnp.float32)
    stored_inputs = normal_values(keys[1], (N_SECTION, TOKENS, D), 1.0, 6.0, ((0, 4), (1, 8)), jnp.float32)
    out_grads = normal_values(keys[2], (N_SECTION, TOKENS, D), 1.0, 6.0, ((0, 4), (1, 8)))
    fwd_routes_keys = jax.random.split(jax.random.fold_in(keys[3], 1), N_SECTION * TOKENS // TOK_DEV)
    fwd_routes_turns = jax.random.permutation(jax.random.fold_in(keys[3], 3), N_SECTION * TOKENS // TOK_DEV)
    fwd_routes = jax.vmap(lambda own, number: routed_block(jax.random.fold_in(keys[3], 2), own, number, TOK_DEV, EXPERTS, 2, CAP, 2))(fwd_routes_keys, fwd_routes_turns).reshape((N_SECTION, TOKENS, 2))
    fwd_gates = jnp.clip(0.2 + 0.8 * jax.random.uniform(keys[4], (N_SECTION, TOKENS, 2), jnp.float32) ** levels(keys[4], (N_SECTION, TOKENS, 2), ((0, 4), (1, 8)), -0.2, 0.2), 0.2, 1.0)
    fwd_modulation = normal_values(keys[5], (N_SECTION, 3, D), 0.5, 3.0, ((0, 4),), jnp.float32)
    bwd_routes_keys = jax.random.split(jax.random.fold_in(keys[6], 1), N_SECTION * TOKENS // TOK_DEV)
    bwd_routes_turns = jax.random.permutation(jax.random.fold_in(keys[6], 3), N_SECTION * TOKENS // TOK_DEV)
    bwd_routes = jax.vmap(lambda own, number: routed_block(jax.random.fold_in(keys[6], 2), own, number, TOK_DEV, EXPERTS, 2, CAP, 2))(bwd_routes_keys, bwd_routes_turns).reshape((N_SECTION, TOKENS, 2))
    bwd_gates = jnp.clip(0.2 + 0.8 * jax.random.uniform(keys[7], (N_SECTION, TOKENS, 2), jnp.float32) ** levels(keys[7], (N_SECTION, TOKENS, 2), ((0, 4), (1, 8)), -0.2, 0.2), 0.2, 1.0)
    bwd_modulation = normal_values(keys[8], (N_SECTION, 3, D), 0.5, 3.0, ((0, 4),), jnp.float32)
    up_weight = normal_values(keys[9], (N_SECTION, N_EXPERT, D, FF_DEV), D ** -0.5, 0.125, ((0, 4), (1, 8)))
    down_weight = normal_values(keys[10], (N_SECTION, N_EXPERT, FF_DEV, D), FF ** -0.5, 0.125, ((0, 4), (1, 8)))
    return dict(section_inputs=section_inputs, stored_inputs=stored_inputs, out_grads=out_grads, fwd_routes=fwd_routes, fwd_gates=fwd_gates, fwd_modulation=fwd_modulation, bwd_routes=bwd_routes, bwd_gates=bwd_gates, bwd_modulation=bwd_modulation, up_weight=up_weight, down_weight=down_weight)


norm_eps = 1e-06

def layer_norm(tok_rows):
    mean_row = lax.optimization_barrier(jnp.mean(tok_rows, axis=-1, keepdims=True))
    centered = tok_rows - mean_row
    variance = lax.optimization_barrier(jnp.mean(centered * centered, axis=-1, keepdims=True))
    inv_std = lax.rsqrt(variance + norm_eps)
    return (centered * inv_std, inv_std)

def slot_numbers(routes):
    flat_ids = routes.reshape(-1).astype(jnp.int32)
    choose = (flat_ids[:, None] == jnp.arange(EXPERTS, dtype=jnp.int32)[None, :]).astype(jnp.int32)
    before = jnp.cumsum(choose, axis=0) - choose
    return (flat_ids, lax.optimization_barrier(jnp.sum(before * choose, axis=1)).astype(jnp.int32))

def place_rows(flat_ids, slot_index, pair_values):
    empty = jnp.zeros((EXPERTS, N_EXPERT * CAP, D), pair_values.dtype)
    return empty.at[flat_ids, slot_index].set(pair_values)

def one_section(packed):
    inputs, stored, grads, fwd_routes, fwd_gates, fwd_mod, bwd_routes, bwd_gates, bwd_mod, up_w, down_w = packed
    up_all = up_w.reshape(EXPERTS, 2, D, FF_DEV).astype(jnp.float32)
    down_all = down_w.reshape(EXPERTS, 2, FF_DEV, D).astype(jnp.float32)
    normed, _ = layer_norm(inputs)
    hidden = (normed * (1.0 + fwd_mod[1]) + fwd_mod[0]).astype(jnp.bfloat16)
    flat_ids, slot_index = slot_numbers(fwd_routes)
    rows = place_rows(flat_ids, slot_index, jnp.repeat(hidden, 2, axis=0)).astype(jnp.float32)
    pre_act = jnp.einsum('erd,ejdf->ejrf', rows, up_all)
    activation = jax.nn.gelu(pre_act).astype(jnp.bfloat16).astype(jnp.float32)
    partial_value = jnp.einsum('ejrf,ejfd->ejrd', activation, down_all).astype(jnp.bfloat16).astype(jnp.float32)
    summed = partial_value[:, 0] + partial_value[:, 1]
    pair_out = summed[flat_ids, slot_index].reshape(TOKENS, 2, D)
    moe_out = lax.optimization_barrier(jnp.sum(pair_out * fwd_gates[:, :, None], axis=1))
    out_fwd = inputs + fwd_mod[2] * moe_out
    normed_b, inv_b = layer_norm(stored)
    hidden_b = (normed_b * (1.0 + bwd_mod[1]) + bwd_mod[0]).astype(jnp.bfloat16)
    grad_rows = grads.astype(jnp.float32)
    pair_grads = (bwd_gates[:, :, None] * (bwd_mod[2] * grad_rows)[:, None, :]).astype(jnp.bfloat16).reshape(2 * TOKENS, D)
    flat_b, slot_b = slot_numbers(bwd_routes)
    rows_h = place_rows(flat_b, slot_b, jnp.repeat(hidden_b, 2, axis=0)).astype(jnp.float32)
    rows_g = place_rows(flat_b, slot_b, pair_grads).astype(jnp.float32)
    pre_b = jnp.einsum('erd,ejdf->ejrf', rows_h, up_all)
    act_grad = jnp.einsum('erd,ejfd->ejrf', rows_g, down_all)
    pre_grad = jax.vjp(jax.nn.gelu, pre_b)[1](act_grad)[0].astype(jnp.bfloat16).astype(jnp.float32)
    part_b = jnp.einsum('ejrf,ejdf->ejrd', pre_grad, up_all).astype(jnp.bfloat16).astype(jnp.float32)
    summed_b = part_b[:, 0] + part_b[:, 1]
    dhidden = lax.optimization_barrier(jnp.sum(summed_b[flat_b, slot_b].reshape(TOKENS, 2, D), axis=1))
    dnorm = dhidden * (1.0 + bwd_mod[1])
    mean_one = lax.optimization_barrier(jnp.mean(dnorm, axis=-1, keepdims=True))
    mean_two = lax.optimization_barrier(jnp.mean(dnorm * normed_b, axis=-1, keepdims=True))
    section_grad = (grad_rows + (dnorm - mean_one - normed_b * mean_two) * inv_b).astype(jnp.bfloat16)
    return (out_fwd, section_grad)

def reference(section_inputs, stored_inputs, out_grads, fwd_routes, fwd_gates, fwd_modulation, bwd_routes, bwd_gates, bwd_modulation, up_weight, down_weight):
    out_fwd, section_grad = lax.map(one_section, (section_inputs, stored_inputs, out_grads, fwd_routes, fwd_gates, fwd_modulation, bwd_routes, bwd_gates, bwd_modulation, up_weight, down_weight))
    next_inputs = jnp.concatenate([jnp.zeros_like(out_fwd[:1]), out_fwd[:-1]], axis=0)
    input_grads = jnp.concatenate([section_grad[1:], jnp.zeros_like(section_grad[:1])], axis=0)
    return (next_inputs, input_grads)
```

```python
import functools

import jax
import jax.numpy as jnp
from jax import lax
from jax.experimental import pallas as pl
from jax.experimental.pallas import tpu as pltpu
from jax.sharding import PartitionSpec as P

norm_eps = 1e-06
F32, BF16 = jnp.float32, jnp.bfloat16
MESH = pl.DeviceIdType.MESH
ROOT, CUBE = 0.7978845608028654, 0.044715


def flip(index, mask, bits):
    total = 0
    for b in range(bits):
        bit = (index // (1 << b)) % 2
        total = total + (1 << b) * (1 - bit if mask >> b & 1 else bit)
    return total


def dot(a, b, ca=1, cb=0):
    return lax.dot_general(a, b, (((ca,), (cb,)), ((), ())), preferred_element_type=F32)


def slot_masks(routes, capacity, slots):
    count = routes.shape[0]
    lanes = lax.broadcasted_iota(jnp.int32, (count, 128), 1)
    hits = [routes[:, k : k + 1] == lanes for k in range(2)]
    choose = jnp.where(hits[0] | hits[1], 1.0, 0.0).astype(BF16)
    row = lax.broadcasted_iota(jnp.int32, (count, count), 0)
    col = lax.broadcasted_iota(jnp.int32, (count, count), 1)
    before = dot(jnp.where(col < row, 1.0, 0.0).astype(BF16), choose)
    places = lax.broadcasted_iota(jnp.int32, (count, slots), 1)
    masks = []
    for k in range(2):
        rank = jnp.sum(jnp.where(hits[k], before, 0.0), axis=1, keepdims=True)
        masks.append(places == routes[:, k : k + 1] * capacity + rank.astype(jnp.int32))
    return masks


def kernel(
    sections, units, capacity,
    x_ref, st_ref, og_ref, fr_ref, fg_ref, fm_ref, br_ref, bg_ref, bm_ref, up_hbm, down_hbm,
    next_ref, grad_ref,
    up, down, snd_f, snd_r, snd_g, rcv_f, rcv_r, rcv_g, act, dgelu,
    px_f, px_b, pin_f, pin_b, ret_f, ret_b, rr_f, rr_b,
    hid, pair0, pair1, normed_b, inv_b, out_f, dh, out_b,
    w_sem, in_send, in_recv, fw_send, fw_recv, px_send, px_recv, rt_send, rt_recv,
    sf_send, sf_recv, sb_send, sb_recv,
):
    s, me = lax.axis_index("section"), lax.axis_index("expert")
    experts = units // 2
    bits = units.bit_length() - 1
    chip, core = me // 2, me % 2
    count, width = x_ref.shape
    half = width // 2
    hidden_units = up.shape[1]
    rows = units * capacity
    slots = experts * capacity
    tile = 256
    group = 16
    order = list(reversed(range(1, units)))
    peer = {k: flip(me, k, bits) for k in order}

    w_up = pltpu.make_async_copy(up_hbm, up, w_sem.at[0])
    w_down = pltpu.make_async_copy(down_hbm, down, w_sem.at[1])
    w_up.start()
    w_down.start()

    barrier = pltpu.get_barrier_semaphore()
    for k in order:
        pl.semaphore_signal(barrier, inc=1, device_id=(s, peer[k]), device_id_type=MESH)
    for step in (1, sections - 1):
        pl.semaphore_signal(
            barrier, inc=1, device_id=((s + step) % sections, me), device_id_type=MESH
        )

    def remote(src, dst, send, recv, section, unit):
        return pltpu.make_async_remote_copy(
            src_ref=src, dst_ref=dst, send_sem=send, recv_sem=recv,
            device_id=(section, unit), device_id_type=MESH,
        )

    def inbound(phase, snd, rcv):
        copies = {}
        for k in order:
            d = peer[k]
            if k == 1:
                src, dst = snd.at[chip], rcv.at[:, me]
            else:
                src, dst = snd.at[d // 2, d % 2], rcv.at[d % 2, me]
            copies[k] = remote(src, dst, in_send.at[phase, k], in_recv.at[phase, k], s, d)
        return copies

    def hand_on(phase, rcv):
        copies = {}
        for k in order:
            if k > 1:
                block = rcv.at[core, peer[k]]
                copies[k] = remote(
                    block, block, fw_send.at[phase, k], fw_recv.at[phase, k], s, peer[1]
                )
        return copies

    def keep_own(snd, rcv):
        for h in range(2):
            rcv[h, me] = snd[chip, h]

    def receive(ins, fws):
        for k in order:
            ins[k].wait_recv()
            if k > 1:
                fws[k].start()
        for k in order:
            if k > 1:
                fws[k].wait_recv()

    def normalise(src, mod, keep):
        @pl.loop(0, count // group)
        def _(i):
            at = pl.ds(pl.multiple_of(i * group, group), group)
            x = src[at, :]
            centered = x - jnp.mean(x, axis=1, keepdims=True)
            inv = lax.rsqrt(jnp.mean(centered * centered, axis=1, keepdims=True) + norm_eps)
            normed = centered * inv
            hid[at, :] = (normed * (1.0 + mod[1:2, :]) + mod[0:1, :]).astype(BF16)
            if keep:
                normed_b[at, :] = normed
                inv_b[at, :] = jnp.broadcast_to(inv, (group, 128))

    def pack(terms, snd):
        for h in range(2):
            @pl.loop(0, half // tile)
            def _(n):
                src = pl.ds(pl.multiple_of(h * half + n * tile, tile), tile)
                value = sum(dot(mask, ref[:, src], 0, 0) for mask, ref in terms).astype(BF16)
                for e in range(experts):
                    snd[e, h, :, pl.ds(pl.multiple_of(n * tile, tile), tile)] = value[
                        e * capacity : (e + 1) * capacity, :
                    ]

    def onehot(mask):
        return jnp.where(mask, 1.0, 0.0).astype(BF16)

    normalise(x_ref, fm_ref, False)
    fwd = slot_masks(fr_ref[...], capacity, slots)
    pack([(onehot(fwd[0] | fwd[1]), hid)], snd_f)
    pl.semaphore_wait(barrier, units + 1)
    in_f, fw_f = inbound(0, snd_f, rcv_f), hand_on(0, rcv_f)
    for k in order:
        in_f[k].start()
    keep_own(snd_f, rcv_f)

    normalise(st_ref, bm_ref, True)
    bwd = slot_masks(br_ref[...], capacity, slots)
    bwd_hot = [onehot(mask) for mask in bwd]
    pack([(bwd_hot[0] + bwd_hot[1], hid)], snd_r)
    in_r, fw_r = inbound(1, snd_r, rcv_r), hand_on(1, rcv_r)
    for k in order:
        in_r[k].start()
    keep_own(snd_r, rcv_r)

    @pl.loop(0, count // group)
    def _(i):
        at = pl.ds(pl.multiple_of(i * group, group), group)
        scaled = bm_ref[2:3, :] * og_ref[at, :].astype(F32)
        pair0[at, :] = (bg_ref[at, 0:1] * scaled).astype(BF16)
        pair1[at, :] = (bg_ref[at, 1:2] * scaled).astype(BF16)

    pack([(bwd_hot[0], pair0), (bwd_hot[1], pair1)], snd_g)
    in_g, fw_g = inbound(2, snd_g, rcv_g), hand_on(2, rcv_g)
    for k in order:
        in_g[k].start()
    keep_own(snd_g, rcv_g)

    def flat(ref, h):
        return ref[h].reshape(rows, half)

    def cols(n, base=0):
        return pl.ds(pl.multiple_of(base + n * tile, tile), tile)

    def exchange(phase, px, pin, ret, result):
        def fill(dst, h):
            @pl.loop(0, half // tile)
            def _(n):
                value = result(h, n).astype(BF16).reshape(units, capacity, tile)
                dst[:, :, cols(n)] = value

        fill(px, 1 - core)
        swap = remote(px, pin, px_send.at[phase], px_recv.at[phase], s, peer[1])
        swap.start()
        fill(ret, core)
        swap.wait_recv()

        @pl.loop(0, units)
        def _(u):
            ret[u] = (ret[u].astype(F32) + pin[u].astype(F32)).astype(BF16)

        return swap

    def give_back(phase, ret, rr):
        copies = {}
        for k in order:
            copies[k] = remote(
                ret.at[peer[k]], rr.at[core, chip],
                rt_send.at[phase, k], rt_recv.at[phase, k], s, peer[k],
            )
            copies[k].start()
        rr[core, chip] = ret[me]
        return copies

    receive(in_f, fw_f)
    w_up.wait()
    w_down.wait()

    @pl.loop(0, hidden_units // tile)
    def _(n):
        pre = dot(flat(rcv_f, 0), up[:half, cols(n)]) + dot(flat(rcv_f, 1), up[half:, cols(n)])
        t = jnp.tanh(ROOT * (pre + CUBE * pre * pre * pre))
        act[:, cols(n)] = (0.5 * pre * (1.0 + t)).astype(BF16)

    swap_f = exchange(
        0, px_f, pin_f, ret_f, lambda h, n: dot(act[...], down[:, cols(n, h * half)])
    )
    back_f = give_back(0, ret_f, rr_f)

    receive(in_r, fw_r)

    @pl.loop(0, hidden_units // tile)
    def _(n):
        pre = dot(flat(rcv_r, 0), up[:half, cols(n)]) + dot(flat(rcv_r, 1), up[half:, cols(n)])
        t = jnp.tanh(ROOT * (pre + CUBE * pre * pre * pre))
        slope = ROOT * (1.0 + 3.0 * CUBE * pre * pre)
        dgelu[:, cols(n)] = 0.5 * (1.0 + t) + 0.5 * pre * (1.0 - t * t) * slope

    receive(in_g, fw_g)

    @pl.loop(0, hidden_units // tile)
    def _(n):
        back = dot(flat(rcv_g, 0), down[cols(n), :half], 1, 1) + dot(
            flat(rcv_g, 1), down[cols(n), half:], 1, 1
        )
        act[:, cols(n)] = (back * dgelu[:, cols(n)]).astype(BF16)

    swap_b = exchange(
        1, px_b, pin_b, ret_b, lambda h, n: dot(act[...], up[cols(n, h * half), :], 1, 1)
    )
    back_b = give_back(1, ret_b, rr_b)

    weight = sum(jnp.where(fwd[k], fg_ref[:, k : k + 1], 0.0) for k in range(2))
    high = weight.astype(BF16)
    low = (weight - high.astype(F32)).astype(BF16)
    for k in order:
        back_f[k].wait_recv()
    sends_f = []
    for h in range(2):
        side = pl.ds(h * half, half)

        @pl.loop(0, half // tile)
        def _(n):
            got = rr_f[h, :, :, cols(n)].reshape(slots, tile)
            moe = dot(high, got) + dot(low, got)
            at = cols(n, h * half)
            out_f[:, at] = x_ref[:, at] + fm_ref[2:3, at] * moe

        copy = remote(
            out_f.at[:, side], next_ref.at[:, side], sf_send.at[h], sf_recv.at[h],
            (s + 1) % sections, me,
        )
        sends_f.append(copy)

        @pl.when(s < sections - 1)
        def _():
            copy.start()

    @pl.when(s == 0)
    def _():
        next_ref[...] = jnp.zeros_like(next_ref)

    @pl.when(s == sections - 1)
    def _():
        grad_ref[...] = jnp.zeros_like(grad_ref)

    for k in order:
        back_b[k].wait_recv()
    both = bwd_hot[0] + bwd_hot[1]
    for h in range(2):
        @pl.loop(0, half // tile)
        def _(n):
            got = rr_b[h, :, :, cols(n)].reshape(slots, tile)
            dh[:, cols(n, h * half)] = dot(both, got)

    pieces = 4
    part = count // pieces
    sends_b = []
    for p in range(pieces):
        @pl.loop(0, part // group)
        def _(i):
            at = pl.ds(pl.multiple_of(p * part + i * group, group), group)
            dnorm = dh[at, :] * (1.0 + bm_ref[1:2, :])
            normed = normed_b[at, :]
            one = jnp.mean(dnorm, axis=1, keepdims=True)
            two = jnp.mean(dnorm * normed, axis=1, keepdims=True)
            out_b[at, :] = (
                og_ref[at, :].astype(F32) + (dnorm - one - normed * two) * inv_b[at, 0:1]
            ).astype(BF16)

        piece = pl.ds(p * part, part)
        copy = remote(
            out_b.at[piece], grad_ref.at[piece], sb_send.at[p], sb_recv.at[p],
            (s + sections - 1) % sections, me,
        )
        sends_b.append(copy)

        @pl.when(s > 0)
        def _():
            copy.start()

    for copies in (in_f, in_r, in_g, fw_f, fw_r, fw_g, back_f, back_b):
        for copy in copies.values():
            copy.wait_send()
    swap_f.wait_send()
    swap_b.wait_send()

    @pl.when(s < sections - 1)
    def _():
        for copy in sends_f:
            copy.wait_send()
        for copy in sends_b:
            copy.wait_recv()

    @pl.when(s > 0)
    def _():
        for copy in sends_f:
            copy.wait_recv()
        for copy in sends_b:
            copy.wait_send()


def on_device(
    section_inputs,
    stored_inputs,
    out_grads,
    fwd_routes,
    fwd_gates,
    fwd_modulation,
    bwd_routes,
    bwd_gates,
    bwd_modulation,
    up_weight,
    down_weight,
):
    sections, units = lax.axis_size("section"), lax.axis_size("expert")
    experts = units // 2
    count, width = section_inputs.shape[1:]
    hidden_units = up_weight.shape[3]
    half = width // 2
    capacity = -(-min(count, 5 * count // (2 * experts)) // 16) * 16
    rows = units * capacity

    def vmem(dtype, *shape):
        return pltpu.VMEM(shape, dtype)

    def dma(*shape):
        return pltpu.SemaphoreType.DMA(shape)

    scratch = [
        vmem(BF16, width, hidden_units),
        vmem(BF16, hidden_units, width),
        *[vmem(BF16, experts, 2, capacity, half)] * 3,
        *[vmem(BF16, 2, units, capacity, half)] * 3,
        vmem(BF16, rows, hidden_units),
        vmem(F32, rows, hidden_units),
        *[vmem(BF16, units, capacity, half)] * 6,
        *[vmem(BF16, 2, experts, capacity, half)] * 2,
        *[vmem(BF16, count, width)] * 3,
        vmem(F32, count, width),
        vmem(F32, count, 128),
        *[vmem(F32, count, width)] * 2,
        vmem(BF16, count, width),
        dma(2),
        *[dma(3, units)] * 4,
        *[dma(2)] * 2,
        *[dma(2, units)] * 2,
        *[dma(2)] * 2,
        *[dma(4)] * 2,
    ]
    in_vmem = pl.BlockSpec(memory_space=pltpu.VMEM)
    in_hbm = pl.BlockSpec(memory_space=pl.ANY)
    flops = 10 * rows * width * hidden_units
    next_inputs, input_grads = pl.pallas_call(
        functools.partial(kernel, sections, units, capacity),
        out_shape=(
            jax.ShapeDtypeStruct((count, width), F32),
            jax.ShapeDtypeStruct((count, width), BF16),
        ),
        in_specs=[in_vmem] * 9 + [in_hbm] * 2,
        out_specs=(in_vmem, in_vmem),
        scratch_shapes=scratch,
        compiler_params=pltpu.CompilerParams(
            collective_id=0, has_side_effects=True, vmem_limit_bytes=67043328
        ),
        cost_estimate=pl.CostEstimate(
            flops=flops, bytes_accessed=4 * width * hidden_units, transcendentals=0
        ),
    )(
        section_inputs[0], stored_inputs[0], out_grads[0], fwd_routes[0], fwd_gates[0],
        fwd_modulation[0], bwd_routes[0], bwd_gates[0], bwd_modulation[0],
        up_weight[0, 0], down_weight[0, 0],
    )
    return next_inputs[None], input_grads[None]


def solution(mesh):
    tokens = P("section", "expert", None)
    shared = P("section", None, None)
    weights = P("section", "expert", None, None)
    placed = (tokens,) * 5 + (shared,) + (tokens,) * 2 + (shared,) + (weights,) * 2
    return jax.shard_map(
        on_device,
        mesh=mesh,
        in_specs=placed,
        out_specs=(tokens, tokens),
        check_vma=False,
    )
```

```python
import functools

import jax
import jax.numpy as jnp
from jax import lax
from jax.experimental import pallas as pl
from jax.experimental.pallas import tpu as pltpu
from jax.sharding import PartitionSpec as P

norm_eps = 1e-06
F32, BF16 = jnp.float32, jnp.bfloat16
MESH = pl.DeviceIdType.MESH
ROOT, CUBE = 0.7978845608028654, 0.044715


def flip(index, mask, bits):
    total = 0
    for b in range(bits):
        bit = (index // (1 << b)) % 2
        total = total + (1 << b) * (1 - bit if mask >> b & 1 else bit)
    return total


def dot(a, b, ca=1, cb=0):
    return lax.dot_general(a, b, (((ca,), (cb,)), ((), ())), preferred_element_type=F32)


def slot_masks(routes, capacity, slots):
    count = routes.shape[0]
    lanes = lax.broadcasted_iota(jnp.int32, (count, 128), 1)
    hits = [routes[:, k : k + 1] == lanes for k in range(2)]
    choose = jnp.where(hits[0] | hits[1], 1.0, 0.0).astype(BF16)
    row = lax.broadcasted_iota(jnp.int32, (count, count), 0)
    col = lax.broadcasted_iota(jnp.int32, (count, count), 1)
    before = dot(jnp.where(col < row, 1.0, 0.0).astype(BF16), choose)
    places = lax.broadcasted_iota(jnp.int32, (count, slots), 1)
    masks = []
    for k in range(2):
        rank = jnp.sum(jnp.where(hits[k], before, 0.0), axis=1, keepdims=True)
        masks.append(places == routes[:, k : k + 1] * capacity + rank.astype(jnp.int32))
    return masks


def kernel(
    sections, units, capacity,
    x_ref, st_ref, og_ref, fr_ref, fg_ref, fm_ref, br_ref, bg_ref, bm_ref, up_hbm, down_hbm,
    next_ref, grad_ref,
    up, down, snd_f, snd_r, snd_g, rcv_f, rcv_r, rcv_g, act, dgelu,
    px_f, px_b, pin_f, pin_b, ret_f, ret_b, rr_f, rr_b,
    hid, pair0, pair1, normed_b, inv_b, out_f, dh, out_b,
    w_sem, in_send, in_recv, fw_send, fw_recv, px_send, px_recv, rt_send, rt_recv,
    sf_send, sf_recv, sb_send, sb_recv,
):
    s, me = lax.axis_index("section"), lax.axis_index("expert")
    experts = units // 2
    bits = units.bit_length() - 1
    chip, core = me // 2, me % 2
    count, width = x_ref.shape
    half = width // 2
    hidden_units = up.shape[1]
    rows = units * capacity
    slots = experts * capacity
    tile = 256
    group = 16
    order = list(range(1, units))
    peer = {k: flip(me, k, bits) for k in order}

    w_up = pltpu.make_async_copy(up_hbm, up, w_sem.at[0])
    w_down = pltpu.make_async_copy(down_hbm, down, w_sem.at[1])
    w_up.start()
    w_down.start()

    barrier = pltpu.get_barrier_semaphore()
    for k in order:
        pl.semaphore_signal(barrier, inc=1, device_id=(s, peer[k]), device_id_type=MESH)
    for step in (1, sections - 1):
        pl.semaphore_signal(
            barrier, inc=1, device_id=((s + step) % sections, me), device_id_type=MESH
        )

    def remote(src, dst, send, recv, section, unit):
        return pltpu.make_async_remote_copy(
            src_ref=src, dst_ref=dst, send_sem=send, recv_sem=recv,
            device_id=(section, unit), device_id_type=MESH,
        )

    def inbound(phase, snd, rcv):
        copies = {}
        for k in order:
            d = peer[k]
            if k == 1:
                src, dst = snd.at[chip], rcv.at[:, me]
            else:
                src, dst = snd.at[d // 2, d % 2], rcv.at[d % 2, me]
            copies[k] = remote(src, dst, in_send.at[phase, k], in_recv.at[phase, k], s, d)
        return copies

    def hand_on(phase, rcv):
        copies = {}
        for k in order:
            if k > 1:
                block = rcv.at[core, peer[k]]
                copies[k] = remote(
                    block, block, fw_send.at[phase, k], fw_recv.at[phase, k], s, peer[1]
                )
        return copies

    def keep_own(snd, rcv):
        for h in range(2):
            rcv[h, me] = snd[chip, h]

    def receive(ins, fws):
        for k in order:
            ins[k].wait_recv()
            if k > 1:
                fws[k].start()
        for k in order:
            if k > 1:
                fws[k].wait_recv()

    def normalise(src, mod, keep):
        @pl.loop(0, count // group)
        def _(i):
            at = pl.ds(pl.multiple_of(i * group, group), group)
            x = src[at, :]
            centered = x - jnp.mean(x, axis=1, keepdims=True)
            inv = lax.rsqrt(jnp.mean(centered * centered, axis=1, keepdims=True) + norm_eps)
            normed = centered * inv
            hid[at, :] = (normed * (1.0 + mod[1:2, :]) + mod[0:1, :]).astype(BF16)
            if keep:
                normed_b[at, :] = normed
                inv_b[at, :] = jnp.broadcast_to(inv, (group, 128))

    def pack(terms, snd):
        for h in range(2):
            @pl.loop(0, half // tile)
            def _(n):
                src = pl.ds(pl.multiple_of(h * half + n * tile, tile), tile)
                value = sum(dot(mask, ref[:, src], 0, 0) for mask, ref in terms).astype(BF16)
                for e in range(experts):
                    snd[e, h, :, pl.ds(pl.multiple_of(n * tile, tile), tile)] = value[
                        e * capacity : (e + 1) * capacity, :
                    ]

    def onehot(mask):
        return jnp.where(mask, 1.0, 0.0).astype(BF16)

    normalise(x_ref, fm_ref, False)
    fwd = slot_masks(fr_ref[...], capacity, slots)
    pack([(onehot(fwd[0] | fwd[1]), hid)], snd_f)
    pl.semaphore_wait(barrier, units + 1)
    in_f, fw_f = inbound(0, snd_f, rcv_f), hand_on(0, rcv_f)
    for k in order:
        in_f[k].start()
    keep_own(snd_f, rcv_f)

    normalise(st_ref, bm_ref, True)
    bwd = slot_masks(br_ref[...], capacity, slots)
    bwd_hot = [onehot(mask) for mask in bwd]
    pack([(bwd_hot[0] + bwd_hot[1], hid)], snd_r)
    in_r, fw_r = inbound(1, snd_r, rcv_r), hand_on(1, rcv_r)
    for k in order:
        in_r[k].start()
    keep_own(snd_r, rcv_r)

    @pl.loop(0, count // group)
    def _(i):
        at = pl.ds(pl.multiple_of(i * group, group), group)
        scaled = bm_ref[2:3, :] * og_ref[at, :].astype(F32)
        pair0[at, :] = (bg_ref[at, 0:1] * scaled).astype(BF16)
        pair1[at, :] = (bg_ref[at, 1:2] * scaled).astype(BF16)

    pack([(bwd_hot[0], pair0), (bwd_hot[1], pair1)], snd_g)
    in_g, fw_g = inbound(2, snd_g, rcv_g), hand_on(2, rcv_g)
    for k in order:
        in_g[k].start()
    keep_own(snd_g, rcv_g)

    def flat(ref, h):
        return ref[h].reshape(rows, half)

    def cols(n, base=0):
        return pl.ds(pl.multiple_of(base + n * tile, tile), tile)

    def exchange(phase, px, pin, ret, result):
        def fill(dst, h):
            @pl.loop(0, half // tile)
            def _(n):
                value = result(h, n).astype(BF16).reshape(units, capacity, tile)
                dst[:, :, cols(n)] = value

        fill(px, 1 - core)
        swap = remote(px, pin, px_send.at[phase], px_recv.at[phase], s, peer[1])
        swap.start()
        fill(ret, core)
        swap.wait_recv()

        @pl.loop(0, units)
        def _(u):
            ret[u] = (ret[u].astype(F32) + pin[u].astype(F32)).astype(BF16)

        return swap

    def give_back(phase, ret, rr):
        copies = {}
        for k in order:
            copies[k] = remote(
                ret.at[peer[k]], rr.at[core, chip],
                rt_send.at[phase, k], rt_recv.at[phase, k], s, peer[k],
            )
            copies[k].start()
        rr[core, chip] = ret[me]
        return copies

    receive(in_f, fw_f)
    w_up.wait()
    w_down.wait()

    @pl.loop(0, hidden_units // tile)
    def _(n):
        pre = dot(flat(rcv_f, 0), up[:half, cols(n)]) + dot(flat(rcv_f, 1), up[half:, cols(n)])
        t = jnp.tanh(ROOT * (pre + CUBE * pre * pre * pre))
        act[:, cols(n)] = (0.5 * pre * (1.0 + t)).astype(BF16)

    swap_f = exchange(
        0, px_f, pin_f, ret_f, lambda h, n: dot(act[...], down[:, cols(n, h * half)])
    )
    back_f = give_back(0, ret_f, rr_f)

    receive(in_r, fw_r)

    @pl.loop(0, hidden_units // tile)
    def _(n):
        pre = dot(flat(rcv_r, 0), up[:half, cols(n)]) + dot(flat(rcv_r, 1), up[half:, cols(n)])
        t = jnp.tanh(ROOT * (pre + CUBE * pre * pre * pre))
        slope = ROOT * (1.0 + 3.0 * CUBE * pre * pre)
        dgelu[:, cols(n)] = 0.5 * (1.0 + t) + 0.5 * pre * (1.0 - t * t) * slope

    receive(in_g, fw_g)

    @pl.loop(0, hidden_units // tile)
    def _(n):
        back = dot(flat(rcv_g, 0), down[cols(n), :half], 1, 1) + dot(
            flat(rcv_g, 1), down[cols(n), half:], 1, 1
        )
        act[:, cols(n)] = (back * dgelu[:, cols(n)]).astype(BF16)

    swap_b = exchange(
        1, px_b, pin_b, ret_b, lambda h, n: dot(act[...], up[cols(n, h * half), :], 1, 1)
    )
    back_b = give_back(1, ret_b, rr_b)

    weight = sum(jnp.where(fwd[k], fg_ref[:, k : k + 1], 0.0) for k in range(2))
    high = weight.astype(BF16)
    low = (weight - high.astype(F32)).astype(BF16)
    for k in order:
        back_f[k].wait_recv()
    sends_f = []
    for h in range(2):
        side = pl.ds(h * half, half)

        @pl.loop(0, half // tile)
        def _(n):
            got = rr_f[h, :, :, cols(n)].reshape(slots, tile)
            moe = dot(high, got) + dot(low, got)
            at = cols(n, h * half)
            out_f[:, at] = x_ref[:, at] + fm_ref[2:3, at] * moe

        copy = remote(
            out_f.at[:, side], next_ref.at[:, side], sf_send.at[h], sf_recv.at[h],
            (s + 1) % sections, me,
        )
        sends_f.append(copy)

        @pl.when(s < sections - 1)
        def _():
            copy.start()

    @pl.when(s == 0)
    def _():
        next_ref[...] = jnp.zeros_like(next_ref)

    @pl.when(s == sections - 1)
    def _():
        grad_ref[...] = jnp.zeros_like(grad_ref)

    for k in order:
        back_b[k].wait_recv()
    both = bwd_hot[0] + bwd_hot[1]
    for h in range(2):
        @pl.loop(0, half // tile)
        def _(n):
            got = rr_b[h, :, :, cols(n)].reshape(slots, tile)
            dh[:, cols(n, h * half)] = dot(both, got)

    pieces = 4
    part = count // pieces
    sends_b = []
    for p in range(pieces):
        @pl.loop(0, part // group)
        def _(i):
            at = pl.ds(pl.multiple_of(p * part + i * group, group), group)
            dnorm = dh[at, :] * (1.0 + bm_ref[1:2, :])
            normed = normed_b[at, :]
            one = jnp.mean(dnorm, axis=1, keepdims=True)
            two = jnp.mean(dnorm * normed, axis=1, keepdims=True)
            out_b[at, :] = (
                og_ref[at, :].astype(F32) + (dnorm - one - normed * two) * inv_b[at, 0:1]
            ).astype(BF16)

        piece = pl.ds(p * part, part)
        copy = remote(
            out_b.at[piece], grad_ref.at[piece], sb_send.at[p], sb_recv.at[p],
            (s + sections - 1) % sections, me,
        )
        sends_b.append(copy)

        @pl.when(s > 0)
        def _():
            copy.start()

    for copies in (in_f, in_r, in_g, fw_f, fw_r, fw_g, back_f, back_b):
        for copy in copies.values():
            copy.wait_send()
    swap_f.wait_send()
    swap_b.wait_send()

    @pl.when(s < sections - 1)
    def _():
        for copy in sends_f:
            copy.wait_send()
        for copy in sends_b:
            copy.wait_recv()

    @pl.when(s > 0)
    def _():
        for copy in sends_f:
            copy.wait_recv()
        for copy in sends_b:
            copy.wait_send()


def on_device(
    section_inputs,
    stored_inputs,
    out_grads,
    fwd_routes,
    fwd_gates,
    fwd_modulation,
    bwd_routes,
    bwd_gates,
    bwd_modulation,
    up_weight,
    down_weight,
):
    sections, units = lax.axis_size("section"), lax.axis_size("expert")
    experts = units // 2
    count, width = section_inputs.shape[1:]
    hidden_units = up_weight.shape[3]
    half = width // 2
    capacity = -(-min(count, 5 * count // (2 * experts)) // 16) * 16
    rows = units * capacity

    def vmem(dtype, *shape):
        return pltpu.VMEM(shape, dtype)

    def dma(*shape):
        return pltpu.SemaphoreType.DMA(shape)

    scratch = [
        vmem(BF16, width, hidden_units),
        vmem(BF16, hidden_units, width),
        *[vmem(BF16, experts, 2, capacity, half)] * 3,
        *[vmem(BF16, 2, units, capacity, half)] * 3,
        vmem(BF16, rows, hidden_units),
        vmem(F32, rows, hidden_units),
        *[vmem(BF16, units, capacity, half)] * 6,
        *[vmem(BF16, 2, experts, capacity, half)] * 2,
        *[vmem(BF16, count, width)] * 3,
        vmem(F32, count, width),
        vmem(F32, count, 128),
        *[vmem(F32, count, width)] * 2,
        vmem(BF16, count, width),
        dma(2),
        *[dma(3, units)] * 4,
        *[dma(2)] * 2,
        *[dma(2, units)] * 2,
        *[dma(2)] * 2,
        *[dma(4)] * 2,
    ]
    in_vmem = pl.BlockSpec(memory_space=pltpu.VMEM)
    in_hbm = pl.BlockSpec(memory_space=pl.ANY)
    flops = 10 * rows * width * hidden_units
    next_inputs, input_grads = pl.pallas_call(
        functools.partial(kernel, sections, units, capacity),
        out_shape=(
            jax.ShapeDtypeStruct((count, width), F32),
            jax.ShapeDtypeStruct((count, width), BF16),
        ),
        in_specs=[in_vmem] * 9 + [in_hbm] * 2,
        out_specs=(in_vmem, in_vmem),
        scratch_shapes=scratch,
        compiler_params=pltpu.CompilerParams(
            collective_id=0, has_side_effects=True, vmem_limit_bytes=67043328
        ),
        cost_estimate=pl.CostEstimate(
            flops=flops, bytes_accessed=4 * width * hidden_units, transcendentals=0
        ),
    )(
        section_inputs[0], stored_inputs[0], out_grads[0], fwd_routes[0], fwd_gates[0],
        fwd_modulation[0], bwd_routes[0], bwd_gates[0], bwd_modulation[0],
        up_weight[0, 0], down_weight[0, 0],
    )
    return next_inputs[None], input_grads[None]


def solution(mesh):
    tokens = P("section", "expert", None)
    shared = P("section", None, None)
    weights = P("section", "expert", None, None)
    placed = (tokens,) * 5 + (shared,) + (tokens,) * 2 + (shared,) + (weights,) * 2
    return jax.shard_map(
        on_device,
        mesh=mesh,
        in_specs=placed,
        out_specs=(tokens, tokens),
        check_vma=False,
    )
```
